32 devices in a mesh: sfc: 8 (over z, x), grp: 4 (over y, core).
Axes of the slice: x: 2, y: 2, z: 4, core: 2. Of those that a mesh axis runs over, the one named last changes fastest.
Arguments:
- tracers: float32 [16, 4, 8, 6144], P(None, None, None, ('sfc', 'grp')), may hold values from 0.05 to 60, as said below
- send_counts: int32 [8, 4, 12], P('sfc', 'grp'), may hold values from 1 to 512, 3072 in all within a row
- point_order: int32 [8, 4, 3072], P('sfc', 'grp'), may hold values from 0 to 3071, each once within a row
- depart_elem: int32 [8, 4, 3, 4, 512], P('sfc', 'grp'), may hold values from 0 to 191
- depart_coords: float32 [8, 4, 2, 3, 4, 512], P('sfc', 'grp'), may hold values from -1 to 1
Outputs:
- transported: float32 [16, 4, 8, 6144], P(None, None, None, ('sfc', 'grp'))
The draws below stay inside these ranges and needn't reach their ends.
Inputs may be any that keep to these rules, and one draw needn't show every extreme that they name: `send_counts`: each row lists, for the 12 owner blocks of one device, how many of its arrival points depart from that owner's elements; a row sums to 3072, and its largest entry is exactly 512. `point_order`: each row is a permutation of the device's arrival points. `tracers`: Positive.
All inputs are finite; a program needn't handle non-finite values.
Results may differ from the reference program's by a relative error of at most 0.0003.
Values sent between devices are 32-bit elements; how exact they have to be, the bound alone decides.
No kernel may reach another device: no remote copies, remote signals or barrier semaphores. Data moves between devices by JAX's collectives and lax.ppermute only.
A program may use at most 64 MiB of HBM per device.

```python
import math
import jax
import jax.numpy as jnp
import numpy as np
from jax import lax

NODES = 16
TRACERS = 8
LEVELS = 4
E_DEV = 192
SEGMENTS = 8
GROUPS = 4
PEERS = 12
POINTS = 3072
CAP = 512
NE = 6144


def draw_tracers(key, part):
    base = jax.random.uniform(jax.random.fold_in(key, 11), (NODES, LEVELS, TRACERS, NE), jnp.float32)
    magnitude = jax.random.uniform(jax.random.fold_in(key, 12), (LEVELS, TRACERS), jnp.float32, 0.3, 0.8)
    flips = jax.random.randint(jax.random.fold_in(key, 13), (LEVELS, TRACERS), 0, 2)
    slope = jnp.where(flips == 0, -magnitude, magnitude)
    node_line = jnp.arange(NODES, dtype=jnp.int32) // 4
    node_x = jnp.array([-1.0, -0.4472135954999579, 0.4472135954999579, 1.0], jnp.float32)[node_line]
    profile = 1.0 + slope[None, :, :, None] * node_x[:, None, None, None]
    device = (jnp.arange(NE, dtype=jnp.int32) // E_DEV).astype(jnp.float32)
    devices = NE // E_DEV
    rising = 1.0 + 2.0 * device / max(devices - 1, 1)
    values = jnp.exp(jnp.log(0.3) + base * (jnp.log(5.0) - jnp.log(0.3)))
    return (values * rising[None, None, None, :] * profile).astype(jnp.float32)


def draw_depart_coords(key, part):
    shape_slots = (SEGMENTS, GROUPS, 3, GROUPS, CAP)
    first_u = jax.random.uniform(jax.random.fold_in(key, 21), shape_slots, jnp.float32)
    second_u = jax.random.uniform(jax.random.fold_in(key, 22), shape_slots, jnp.float32)
    lean = jax.random.uniform(jax.random.fold_in(key, 23), (SEGMENTS, GROUPS, 1, 1, 1), jnp.float32, 0.1, 0.6)
    first = lean + (1.0 - lean) * (2.0 * first_u - 1.0)
    second = 2.0 * second_u - 1.0
    first = jnp.clip(first, -1.0, 1.0)
    return jnp.stack([first, second], 2).astype(jnp.float32)


def set_ends(values, key, smallest, top_value):
    index_at = [jax.random.randint(jax.random.fold_in(key, axis), (), 0, length) for axis, length in enumerate(values.shape)]
    longest = values.shape.index(max(values.shape))
    next_to = index_at[:longest] + [(index_at[longest] + 1) % values.shape[longest]] + index_at[longest + 1:]
    return values.at[tuple(index_at)].set(smallest).at[tuple(next_to)].set(top_value)


def length_profile(count, total, most, skew):
    portions = [(1 << 20) // math.isqrt(grade ** skew) + 1 for grade in range(2, count + 1)]
    rest, holding = total - most - (count - 1), [1] * (count - 1)
    while rest > 0:
        candidates = [i for i in range(count - 1) if holding[i] < most]
        whole, budget = sum([portions[i] for i in candidates]), rest
        for i in candidates:
            more = min(most - holding[i], max(1, budget * portions[i] // whole), rest)
            holding[i] = holding[i] + more
            rest = rest - more
    return np.array([most] + holding)


def uneven(rng, amount, total, limit, skew):
    if amount == 2:
        one = jax.random.randint(rng, (), max(1, total - limit), min(limit, total - 1) + 1)
        return jnp.stack([one, total - one])
    lengths = jnp.asarray(length_profile(amount, total, limit, skew), jnp.int32)
    twos = (amount - 1) // 2
    giver, taker = lengths[1:1 + 2 * twos:2], lengths[2:2 + 2 * twos:2]
    room = jnp.minimum(giver - 1, limit - taker)
    moved = jax.random.randint(jax.random.fold_in(rng, 1), (twos,), 0, 1 << 20) % (room + 1)
    lengths = lengths.at[1:1 + 2 * twos:2].set(giver - moved).at[2:2 + 2 * twos:2].set(taker + moved)
    return lengths[jax.random.permutation(jax.random.fold_in(rng, 2), amount)]


def setup_inputs(seed: int = 0) -> dict:
    keys = jax.random.split(jax.random.key(seed), 6)
    tracers = draw_tracers(jax.random.fold_in(keys[5], 71), 0)
    send_counts = jax.vmap(lambda own: uneven(own, PEERS, NODES * E_DEV, CAP, 2))(jax.random.split(keys[1], SEGMENTS * GROUPS)).reshape((SEGMENTS, GROUPS, PEERS)).astype(jnp.int32)
    point_order = jax.vmap(lambda own: jax.random.permutation(own, NODES * E_DEV))(jax.random.split(keys[2], SEGMENTS * GROUPS)).reshape((SEGMENTS, GROUPS, POINTS)).astype(jnp.int32)
    depart_elem = set_ends(jax.random.randint(keys[3], (SEGMENTS, GROUPS, 3, GROUPS, CAP), 0, E_DEV), jax.random.fold_in(keys[3], 1), 0, E_DEV - 1).astype(jnp.int32)
    depart_coords = draw_depart_coords(jax.random.fold_in(keys[5], 71), 0)
    return dict(tracers=tracers, send_counts=send_counts, point_order=point_order, depart_elem=depart_elem, depart_coords=depart_coords)


NODE_COORD = (-1.0, -0.4472135954999579, 0.4472135954999579, 1.0)
NODE_WEIGHT = (1.0 / 6.0, 5.0 / 6.0, 5.0 / 6.0, 1.0 / 6.0)


def lagrange(coordinate):
    basis_values = []
    for row_node in range(4):
        weighted = jnp.ones_like(coordinate)
        for other_node in range(4):
            if other_node != row_node:
                weighted = weighted * ((coordinate - NODE_COORD[other_node]) / (NODE_COORD[row_node] - NODE_COORD[other_node]))
        basis_values.append(weighted)
    return basis_values


def interpolate(tracer_field, source_row, first, second):
    along_first = lagrange(first)
    along_second = lagrange(second)
    running_sum = None
    for row_node in range(4):
        for column_node in range(4):
            node_plane = jnp.take(tracer_field[4 * row_node + column_node], source_row, axis=1)
            weighted = (along_first[row_node] * along_second[column_node]) * node_plane
            if running_sum is None:
                running_sum, lower_bound, upper_bound = weighted, node_plane, node_plane
            else:
                running_sum = running_sum + weighted
                lower_bound = jnp.minimum(lower_bound, node_plane)
                upper_bound = jnp.maximum(upper_bound, node_plane)
    return jnp.clip(running_sum, lower_bound, upper_bound)


def quad_table():
    return jnp.array([NODE_WEIGHT[a] * NODE_WEIGHT[b] for a in range(4) for b in range(4)], jnp.float32)


def reference(tracers, send_counts, point_order, depart_elem, depart_coords):
    channels = LEVELS * TRACERS
    devices = SEGMENTS * GROUPS
    tracer_field = tracers.reshape(NODES, channels, NE)
    counts_all = send_counts.reshape(devices, PEERS)
    order_all = point_order.reshape(devices, POINTS)
    elem_all = depart_elem.reshape(devices, PEERS, CAP)
    coord_all = depart_coords.reshape(devices, 2, PEERS * CAP)
    slot_index = jnp.arange(CAP, dtype=jnp.int32)
    peer_index = jnp.arange(PEERS, dtype=jnp.int32)
    sfc_side = peer_index // GROUPS
    target = peer_index % GROUPS

    def one_device(device):
        segment = device // GROUPS
        owner_device = ((segment + sfc_side - 1) % SEGMENTS) * GROUPS + target
        counts = counts_all[device]
        offsets = jnp.cumsum(counts) - counts
        source_row = (owner_device[:, None] * E_DEV + elem_all[device]).reshape(-1).astype(jnp.int32)
        coords = coord_all[device]
        values = interpolate(tracer_field, source_row, coords[0], coords[1])
        in_use = slot_index[None, :] < counts[:, None]
        position = jnp.minimum(offsets[:, None] + slot_index[None, :], POINTS - 1).astype(jnp.int32)
        target_point = jnp.where(in_use, order_all[device][position], POINTS).reshape(-1).astype(jnp.int32)
        return jnp.zeros((channels, POINTS), jnp.float32).at[:, target_point].set(values, mode="drop")

    limited = lax.map(one_device, jnp.arange(devices, dtype=jnp.int32))
    limited = limited.reshape(devices, channels, NODES, E_DEV).transpose(2, 1, 0, 3).reshape(NODES, channels, NE)
    quadrature = quad_table()
    old_mass = jnp.sum(jnp.sum(tracer_field, axis=2) * quadrature[:, None], axis=0)
    new_mass = jnp.sum(jnp.sum(limited, axis=2) * quadrature[:, None], axis=0)
    corrected = limited * (old_mass / new_mass)[None, :, None]
    return corrected.reshape(NODES, LEVELS, TRACERS, NE)
```

```python
import functools

import jax
import jax.numpy as jnp
from jax import lax
from jax.experimental import pallas as pl
from jax.experimental.pallas import tpu as pltpu
from jax.sharding import PartitionSpec as P

NODE_COORD = (-1.0, -0.4472135954999579, 0.4472135954999579, 1.0)
NODE_WEIGHT = (1.0 / 6.0, 5.0 / 6.0, 5.0 / 6.0, 1.0 / 6.0)
LANES = 128
VMEM = pltpu.MemorySpace.VMEM
SMEM = pltpu.MemorySpace.SMEM


def passed_along(x, axis, by):
    devices = lax.axis_size(axis)
    return lax.ppermute(x, axis, [(i, (i + by) % devices) for i in range(devices)])


def lagrange(coordinate):
    basis_values = []
    for row_node in range(4):
        weighted = jnp.ones_like(coordinate)
        for other_node in range(4):
            if other_node != row_node:
                weighted = weighted * (
                    (coordinate - NODE_COORD[other_node])
                    * (1.0 / (NODE_COORD[row_node] - NODE_COORD[other_node]))
                )
        basis_values.append(weighted)
    return basis_values


def bf16_parts(x):
    high = x.astype(jnp.bfloat16)
    low = (x - high.astype(jnp.float32)).astype(jnp.bfloat16)
    return high, low


def prep_kernel(elements, counts, order, elem, coords, first, middle, last, node_out, elem_out, padded):
    groups, capacity = elem.shape[1:]
    points = order.shape[1]
    padded[:, :points] = jnp.broadcast_to(order[...], (8, points))
    lane = lax.broadcasted_iota(jnp.int32, (8, capacity), 1)
    width = capacity + LANES
    offset = jnp.int32(0)
    for d, out in enumerate((first, middle, last)):
        for h in range(groups):
            k = d * groups + h
            count = counts[k]
            base = pl.multiple_of(lax.shift_left(lax.shift_right_logical(offset, 7), 7), LANES)
            rest = lax.bitwise_and(offset, LANES - 1)
            window = padded[:, pl.ds(base, width)]
            point = pltpu.roll(window, lax.rem(width - rest, width), 1)[:, :capacity]
            used = lane < count
            node = ((point.astype(jnp.float32) + 0.5) * (1.0 / elements)).astype(jnp.int32)
            at_elem = point - node * elements
            row, column = lax.shift_right_logical(node, 2), lax.bitwise_and(node, 3)
            inner_row = (row == 1) | (row == 2)
            inner_column = (column == 1) | (column == 2)
            weight = jnp.where(inner_row, NODE_WEIGHT[1], NODE_WEIGHT[0]) * jnp.where(
                inner_column, NODE_WEIGHT[1], NODE_WEIGHT[0]
            )
            weight = jnp.where(used, weight, 0.0)
            out[h, 0:1, :] = elem[d, h:h + 1, :].astype(jnp.float32)
            out[h, 1:2, :] = coords[0, d, h:h + 1, :]
            out[h, 2:3, :] = coords[1, d, h:h + 1, :]
            out[h, 3:4, :] = weight[0:1, :]
            node_out[d, h:h + 1, :] = jnp.where(used, node, -1)[0:1, :]
            elem_out[d, h:h + 1, :] = jnp.where(used, at_elem, -1)[0:1, :]
            offset = offset + count


def split_kernel(channels, tracers, high_out, low_out, mass_out):
    x = tracers[...]
    high, low = bf16_parts(x)
    high_out[...] = high
    low_out[...] = low
    total = None
    for node in range(16):
        quadrature = NODE_WEIGHT[node // 4] * NODE_WEIGHT[node % 4]
        term = x[node * channels:(node + 1) * channels, :] * quadrature
        total = term if total is None else total + term
    mass_out[...] = jnp.sum(total, axis=1, keepdims=True) + jnp.zeros((channels, LANES), jnp.float32)


def interp_kernel(channels, high, low, old, queries, values, mass, acc):
    groups, sides, _, capacity = queries.shape
    elements = high.shape[1]
    acc[...] = jnp.zeros_like(acc)
    row = lax.broadcasted_iota(jnp.int32, (elements, capacity), 0).astype(jnp.float32)

    def block(k, carry):
        h, d = lax.div(k, sides), lax.rem(k, sides)
        query = queries[h, d]
        onehot = jnp.where(row == query[0:1, :], 1.0, 0.0).astype(jnp.bfloat16)
        field = jnp.dot(high[...], onehot, preferred_element_type=jnp.float32) + jnp.dot(
            low[...], onehot, preferred_element_type=jnp.float32
        )
        along_first = lagrange(query[1:2, :])
        along_second = lagrange(query[2:3, :])
        total = least = greatest = None
        for node in range(16):
            plane = field[node * channels:(node + 1) * channels, :]
            weighted = (along_first[node // 4] * along_second[node % 4]) * plane
            if total is None:
                total, least, greatest = weighted, plane, plane
            else:
                total = total + weighted
                least = jnp.minimum(least, plane)
                greatest = jnp.maximum(greatest, plane)
        value = jnp.minimum(jnp.maximum(total, least), greatest)
        values[h, d] = value
        acc[...] += value * query[3:4, :]
        return carry

    lax.fori_loop(0, groups * sides, block, 0)
    new = jnp.sum(acc[...], axis=1, keepdims=True) + jnp.zeros((channels, LANES), jnp.float32)
    lane = lax.broadcasted_iota(jnp.int32, (channels, LANES), 1)
    which = lax.broadcasted_iota(jnp.int32, (channels, LANES), 0)
    spread = jnp.where(lane == which, old[...], 0.0) + jnp.where(lane == which + channels, new, 0.0)
    mass[...] = jnp.sum(spread, axis=0, keepdims=True)


def final_kernel(channels, first, middle, last, node, elem, masses, out, acc):
    groups, _, capacity = first.shape
    elements = out.shape[1]
    row = lax.broadcasted_iota(jnp.int32, (elements, capacity), 0)
    acc[...] = jnp.zeros_like(acc)
    for d, values in enumerate((first, middle, last)):
        def block(h, carry):
            high, low = bf16_parts(values[h])
            at_node = jnp.broadcast_to(node[d, pl.ds(h, 1), :].astype(jnp.float32), (channels, capacity)).astype(jnp.bfloat16)
            onehot = jnp.where(row == elem[d, pl.ds(h, 1), :], 1.0, 0.0).astype(jnp.bfloat16)
            zero = jnp.zeros_like(high)
            added = None
            for part in (high, low):
                spread = jnp.concatenate(
                    [jnp.where(at_node == float(n), part, zero) for n in range(16)], 0
                )
                term = lax.dot_general(
                    spread, onehot, (((1,), (1,)), ((), ())), preferred_element_type=jnp.float32
                )
                added = term if added is None else added + term
            acc[...] += added
            return carry

        lax.fori_loop(0, groups, block, 0)
    total = jnp.sum(masses[...], axis=0, keepdims=True)
    lane = lax.broadcasted_iota(jnp.int32, (channels, LANES), 1)
    which = lax.broadcasted_iota(jnp.int32, (channels, LANES), 0)
    old = jnp.sum(jnp.where(lane == which, total, 0.0), axis=1, keepdims=True)
    new = jnp.sum(jnp.where(lane == which + channels, total, 0.0), axis=1, keepdims=True)
    ratio = old / new
    for n in range(16):
        rows = slice(n * channels, (n + 1) * channels)
        out[rows, :] = acc[rows, :] * ratio


def whole(memory=VMEM):
    return pl.BlockSpec(memory_space=memory)


def local(tracers, send_counts, point_order, depart_elem, depart_coords):
    node_count, levels, tracer_count, elements = tracers.shape
    channels = levels * tracer_count
    groups = lax.axis_size("grp")
    devices = lax.axis_size("sfc") * groups
    capacity = depart_elem.shape[-1]
    points = node_count * elements
    f32, i32 = jnp.float32, jnp.int32
    shape = jax.ShapeDtypeStruct

    field = tracers.reshape(node_count * channels, elements)
    first, middle, last, node, elem = pl.pallas_call(
        functools.partial(prep_kernel, elements),
        out_shape=[shape((groups, 4, capacity), f32)] * 3 + [shape((3, groups, capacity), i32)] * 2,
        in_specs=[whole(SMEM)] + [whole()] * 3,
        out_specs=[whole()] * 5,
        scratch_shapes=[pltpu.VMEM((8, points + capacity + LANES), i32)],
        name="prep",
    )(
        send_counts.reshape(-1),
        point_order.reshape(1, points),
        depart_elem.reshape(3, groups, capacity),
        depart_coords.reshape(2, 3, groups, capacity),
    )
    high, low, old = pl.pallas_call(
        functools.partial(split_kernel, channels),
        out_shape=[shape(field.shape, jnp.bfloat16)] * 2 + [shape((channels, LANES), f32)],
        in_specs=[whole()],
        out_specs=[whole()] * 3,
        cost_estimate=pl.CostEstimate(flops=4_000_000, bytes_accessed=1_000_000, transcendentals=0),
        name="split",
    )(field)
    stacked = jnp.stack(
        [passed_along(first, "sfc", -1), middle, passed_along(last, "sfc", 1)], 1
    )
    arrived = lax.all_to_all(stacked, "grp", split_axis=0, concat_axis=0, tiled=True)
    values, mass = pl.pallas_call(
        functools.partial(interp_kernel, channels),
        out_shape=[shape((groups, 3, channels, capacity), f32), shape((1, LANES), f32)],
        in_specs=[whole()] * 4,
        out_specs=[whole()] * 2,
        scratch_shapes=[pltpu.VMEM((channels, capacity), f32)],
        name="interp",
    )(high, low, old, arrived)
    returned = lax.all_to_all(values, "grp", split_axis=0, concat_axis=0, tiled=True)
    from_ahead = passed_along(returned[:, 0], "sfc", 1)
    from_behind = passed_along(returned[:, 2], "sfc", -1)
    copies = jnp.broadcast_to(mass[None], (devices, 1, LANES))
    masses = lax.all_to_all(copies, ("sfc", "grp"), split_axis=0, concat_axis=0, tiled=True)
    out = pl.pallas_call(
        functools.partial(final_kernel, channels),
        out_shape=shape(field.shape, f32),
        in_specs=[whole()] * 6,
        out_specs=whole(),
        scratch_shapes=[pltpu.VMEM(field.shape, f32)],
        name="final",
    )(from_ahead, returned[:, 1], from_behind, node, elem, masses.reshape(devices, LANES))
    return out.reshape(tracers.shape)


def solution(mesh):
    in_specs = (
        P(None, None, None, ("sfc", "grp")),
        P("sfc", "grp", None),
        P("sfc", "grp", None),
        P("sfc", "grp", None, None, None),
        P("sfc", "grp", None, None, None, None),
    )
    out_specs = P(None, None, None, ("sfc", "grp"))
    return jax.shard_map(local, mesh=mesh, in_specs=in_specs, out_specs=out_specs, check_vma=False)
```

```python
import functools

import jax
import jax.numpy as jnp
from jax import lax
from jax.experimental import pallas as pl
from jax.experimental.pallas import tpu as pltpu
from jax.sharding import PartitionSpec as P

NODE_COORD = (-1.0, -0.4472135954999579, 0.4472135954999579, 1.0)
NODE_WEIGHT = (1.0 / 6.0, 5.0 / 6.0, 5.0 / 6.0, 1.0 / 6.0)
LANES = 128
VMEM = pltpu.MemorySpace.VMEM
HBM = pltpu.MemorySpace.HBM


def lagrange(coordinate):
    basis_values = []
    for row_node in range(4):
        weighted = jnp.ones_like(coordinate)
        for other_node in range(4):
            if other_node != row_node:
                weighted = weighted * (
                    (coordinate - NODE_COORD[other_node])
                    * (1.0 / (NODE_COORD[row_node] - NODE_COORD[other_node]))
                )
        basis_values.append(weighted)
    return basis_values


def bf16_parts(x):
    high = x.astype(jnp.bfloat16)
    low = (x - high.astype(jnp.float32)).astype(jnp.bfloat16)
    return high, low


def prep_kernel(elements, counts_in, order_in, elem_in, coords_in, *rest):
    groups, capacity = elem_in.shape[1:]
    chips = groups // 2
    messages, rest = rest[:3 * chips], rest[3 * chips:]
    node_out, elem_out, padded, starts, counts, order, elem, coords, sems = rest
    arrivals = [
        pltpu.make_async_copy(source, target, sems.at[i])
        for i, (source, target) in enumerate(
            ((counts_in, counts), (order_in, order), (elem_in, elem), (coords_in, coords))
        )
    ]
    for arrival in arrivals:
        arrival.start()
    for arrival in arrivals:
        arrival.wait()
    points = order.shape[1]
    padded[:, :points] = jnp.broadcast_to(order[...], (8, points))
    offset = jnp.int32(0)
    for k in range(3 * groups):
        starts[k] = offset
        offset = offset + counts[0, k]
    odd = lax.bitwise_and(lax.axis_index("sfc"), 1)
    me = lax.axis_index("grp")
    chip, core = lax.shift_right_logical(me, 1), lax.bitwise_and(me, 1)
    sides = (2 * odd, 2 - 2 * odd, 1)
    lane = lax.broadcasted_iota(jnp.int32, (8, capacity), 1)
    width = capacity + LANES
    for stage, d in enumerate(sides):
        for hop in range(chips):
            target = lax.rem(chip + hop, chips)
            message = messages[stage * chips + hop]
            for half in range(2):
                h = target * 2 + lax.bitwise_xor(core, half)
                k = d * groups + h
                first, count = starts[k], counts[0, k]
                base = pl.multiple_of(lax.shift_left(lax.shift_right_logical(first, 7), 7), LANES)
                skip = lax.bitwise_and(first, LANES - 1)
                window = padded[:, pl.ds(base, width)]
                point = pltpu.roll(window, lax.rem(width - skip, width), 1)[:, :capacity]
                used = lane < count
                node = ((point.astype(jnp.float32) + 0.5) * (1.0 / elements)).astype(jnp.int32)
                at_elem = point - node * elements
                row, column = lax.shift_right_logical(node, 2), lax.bitwise_and(node, 3)
                inner_row = (row == 1) | (row == 2)
                inner_column = (column == 1) | (column == 2)
                weight = jnp.where(inner_row, NODE_WEIGHT[1], NODE_WEIGHT[0]) * jnp.where(
                    inner_column, NODE_WEIGHT[1], NODE_WEIGHT[0]
                )
                weight = jnp.where(used, weight, 0.0)
                message[half, 0:1, :] = elem[d, pl.ds(h, 1), :].astype(jnp.float32)
                message[half, 1:2, :] = coords[0, d, pl.ds(h, 1), :]
                message[half, 2:3, :] = coords[1, d, pl.ds(h, 1), :]
                message[half, 3:4, :] = weight[0:1, :]
                slot = 2 * hop + half
                node_out[stage, slot:slot + 1, :] = jnp.where(used, node, -1)[0:1, :]
                elem_out[stage, slot:slot + 1, :] = jnp.where(used, at_elem, -1)[0:1, :]


def split_kernel(channels, mine_in, other, high_out, low_out, mass_out, mine, sem):
    arrival = pltpu.make_async_copy(mine_in, mine, sem)
    arrival.start()
    high_out[1], low_out[1] = bf16_parts(other[...])
    arrival.wait()
    high_out[0], low_out[0] = bf16_parts(mine[...])
    total = None
    for node in range(16):
        quadrature = NODE_WEIGHT[node // 4] * NODE_WEIGHT[node % 4]
        term = mine[node * channels:(node + 1) * channels, :] * quadrature
        total = term if total is None else total + term
    mass_out[...] = jnp.sum(total, axis=1, keepdims=True) + jnp.zeros((channels, LANES), jnp.float32)


def lane_sums(x):
    return sum(x[:, i:i + LANES] for i in range(0, x.shape[1], LANES))


def interp_kernel(channels, messages, last, high, low, carried, *rest):
    queries, rest = rest[:messages], rest[messages:]
    if last:
        old, *outs, mass = rest
    else:
        *outs, mass = rest
    elements = high.shape[2]
    capacity = queries[0].shape[-1]
    row = lax.broadcasted_iota(jnp.int32, (elements, capacity), 0).astype(jnp.float32)
    new = carried[...] if carried is not None else jnp.zeros((channels, LANES), jnp.float32)
    for query_ref, out in zip(queries, outs):
        for half in range(2):
            query = query_ref[half]
            onehot = jnp.where(row == query[0:1, :], 1.0, 0.0).astype(jnp.bfloat16)
            field = jnp.dot(high[half], onehot, preferred_element_type=jnp.float32) + jnp.dot(
                low[half], onehot, preferred_element_type=jnp.float32
            )
            along_first = lagrange(query[1:2, :])
            along_second = lagrange(query[2:3, :])
            total = least = greatest = None
            for node in range(16):
                plane = field[node * channels:(node + 1) * channels, :]
                weighted = (along_first[node // 4] * along_second[node % 4]) * plane
                if total is None:
                    total, least, greatest = weighted, plane, plane
                else:
                    total = total + weighted
                    least = jnp.minimum(least, plane)
                    greatest = jnp.maximum(greatest, plane)
            value = jnp.minimum(jnp.maximum(total, least), greatest)
            out[half] = value
            new = new + lane_sums(value * query[3:4, :])
    if not last:
        mass[...] = new
        return
    new = jnp.sum(new, axis=1, keepdims=True) + jnp.zeros((channels, LANES), jnp.float32)
    lane = lax.broadcasted_iota(jnp.int32, (channels, LANES), 1)
    which = lax.broadcasted_iota(jnp.int32, (channels, LANES), 0)
    spread = jnp.where(lane == which, old[...], 0.0) + jnp.where(lane == which + channels, new, 0.0)
    mass[...] = jnp.broadcast_to(jnp.sum(spread, axis=0, keepdims=True), mass.shape)


def scattered(channels, value_refs, node, elem, elements):
    capacity = value_refs[0].shape[-1]
    row = lax.broadcasted_iota(jnp.int32, (elements, capacity), 0)
    total = None
    for i, values in enumerate(value_refs):
        for half in range(2):
            slot = 2 * i + half
            at_node = jnp.broadcast_to(
                node[slot:slot + 1, :].astype(jnp.float32), (channels, capacity)
            ).astype(jnp.bfloat16)
            onehot = jnp.where(row == elem[slot:slot + 1, :], 1.0, 0.0).astype(jnp.bfloat16)
            for part in bf16_parts(values[half]):
                zero = jnp.zeros_like(part)
                spread = jnp.concatenate(
                    [jnp.where(at_node == float(n), part, zero) for n in range(16)], 0
                )
                term = lax.dot_general(
                    spread, onehot, (((1,), (1,)), ((), ())), preferred_element_type=jnp.float32
                )
                total = term if total is None else total + term
    return total


def scatter_kernel(channels, stage, messages, *rest):
    values, (node, elem), rest = rest[:messages], rest[messages:messages + 2], rest[messages + 2:]
    *carried, out = rest
    total = scattered(channels, values, node.at[stage], elem.at[stage], out.shape[1])
    out[...] = total + carried[0][...] if carried else total


def scale_kernel(channels, carried, masses, out):
    total = jnp.sum(masses[...], axis=0, keepdims=True)
    lane = lax.broadcasted_iota(jnp.int32, (channels, LANES), 1)
    which = lax.broadcasted_iota(jnp.int32, (channels, LANES), 0)
    old = jnp.sum(jnp.where(lane == which, total, 0.0), axis=1, keepdims=True)
    new = jnp.sum(jnp.where(lane == which + channels, total, 0.0), axis=1, keepdims=True)
    ratio = old / new
    for n in range(16):
        rows = slice(n * channels, (n + 1) * channels)
        out[rows, :] = carried[rows, :] * ratio


def whole(memory=VMEM):
    return pl.BlockSpec(memory_space=memory)


def call(kernel, name, out_shape, *args, outside=0, scratch=(), flops=1_000_000):
    outs = out_shape if isinstance(out_shape, (list, tuple)) else [out_shape]
    moved = sum(x.size * x.dtype.itemsize for x in list(args) + list(outs))
    return pl.pallas_call(
        kernel,
        out_shape=out_shape,
        in_specs=[whole(HBM)] * outside + [whole()] * (len(args) - outside),
        out_specs=[whole()] * len(outs) if outs is out_shape else whole(),
        scratch_shapes=list(scratch),
        compiler_params=pltpu.CompilerParams(vmem_limit_bytes=16 * 1024 * 1024),
        cost_estimate=pl.CostEstimate(flops=flops, bytes_accessed=moved, transcendentals=0),
        name=name,
    )(*[pltpu.with_memory_space_constraint(x, HBM) if i < outside else x for i, x in enumerate(args)])


def local(tracers, send_counts, point_order, depart_elem, depart_coords):
    node_count, levels, tracer_count, elements = tracers.shape
    channels = levels * tracer_count
    segments, groups = lax.axis_size("sfc"), lax.axis_size("grp")
    chips = groups // 2
    devices = segments * groups
    capacity = depart_elem.shape[-1]
    points = node_count * elements
    f32, i32 = jnp.float32, jnp.int32
    shape = jax.ShapeDtypeStruct
    both = ("sfc", "grp")

    def route(stage, hop, back=False):
        pairs = []
        for s in range(segments):
            t = ((((s + 1) ^ 1) - 1) % segments, s ^ 1, s)[stage]
            for g in range(groups):
                to = ((g // 2 + hop) % chips) * 2 + g % 2
                pairs.append((s * groups + g, t * groups + to))
        return [(b, a) for a, b in pairs] if back else pairs

    def moved(stage, arrays, back=False):
        return [
            x if stage == 2 and hop == 0 else lax.ppermute(x, both, route(stage, hop, back))
            for hop, x in enumerate(arrays)
        ]

    field = tracers.reshape(node_count * channels, elements)
    *messages, node, elem = call(
        functools.partial(prep_kernel, elements),
        "prep",
        [shape((2, 4, capacity), f32)] * (3 * chips) + [shape((3, groups, capacity), i32)] * 2,
        send_counts.reshape(1, 3 * groups),
        point_order.reshape(1, points),
        depart_elem.reshape(3, groups, capacity),
        depart_coords.reshape(2, 3, groups, capacity),
        outside=4,
        scratch=[
            pltpu.VMEM((8, points + capacity + LANES), i32),
            pltpu.SMEM((3 * groups,), i32),
            pltpu.SMEM((1, 3 * groups), i32),
            pltpu.VMEM((1, points), i32),
            pltpu.VMEM((3, groups, capacity), i32),
            pltpu.VMEM((2, 3, groups, capacity), f32),
            pltpu.SemaphoreType.DMA((4,)),
        ],
    )
    arrived = [moved(stage, messages[stage * chips:(stage + 1) * chips]) for stage in range(3)]
    other = lax.ppermute(field, "grp", [(i, i ^ 1) for i in range(groups)])
    high, low, old = call(
        functools.partial(split_kernel, channels),
        "split",
        [shape((2,) + field.shape, jnp.bfloat16)] * 2 + [shape((channels, LANES), f32)],
        field,
        other,
        outside=1,
        scratch=[pltpu.VMEM(field.shape, f32), pltpu.SemaphoreType.DMA],
    )
    value_shapes = [shape((2, channels, capacity), f32)] * chips
    new = jnp.zeros((channels, LANES), f32)
    returned = []
    for stage in range(3):
        last = stage == 2
        *values, new = call(
            functools.partial(interp_kernel, channels, chips, last),
            f"interp{stage}",
            value_shapes + [shape((devices if last else channels, LANES), f32)],
            high, low, new, *arrived[stage], *([old] if last else []),
            flops=400_000_000,
        )
        returned.append(moved(stage, values, back=True))
    masses = lax.all_to_all(new.reshape(devices, 1, LANES), both, split_axis=0, concat_axis=0, tiled=True)
    so_far = []
    for stage in range(3):
        so_far = [
            call(
                functools.partial(scatter_kernel, channels, stage, chips),
                f"scatter{stage}",
                shape(field.shape, f32),
                *returned[stage], node, elem, *so_far,
                flops=400_000_000,
            )
        ]
    out = call(
        functools.partial(scale_kernel, channels),
        "scale",
        shape(field.shape, f32),
        *so_far, masses.reshape(devices, LANES),
    )
    return out.reshape(tracers.shape)


def solution(mesh):
    in_specs = (
        P(None, None, None, ("sfc", "grp")),
        P("sfc", "grp", None),
        P("sfc", "grp", None),
        P("sfc", "grp", None, None, None),
        P("sfc", "grp", None, None, None, None),
    )
    out_specs = P(None, None, None, ("sfc", "grp"))
    return jax.shard_map(local, mesh=mesh, in_specs=in_specs, out_specs=out_specs, check_vma=False)
```

```python
import functools

import jax
import jax.numpy as jnp
from jax import lax
from jax.experimental import pallas as pl
from jax.experimental.pallas import tpu as pltpu
from jax.sharding import PartitionSpec as P


NODE_COORD = (-1.0, -0.4472135954999579, 0.4472135954999579, 1.0)
NODE_WEIGHT = (1.0 / 6.0, 5.0 / 6.0, 5.0 / 6.0, 1.0 / 6.0)
LANES = 128
VMEM = pltpu.MemorySpace.VMEM
HBM = pltpu.MemorySpace.HBM
FAR, NEAR, OWN = 0, 1, 2
SCATTERS = (((OWN, 0), (OWN, 2)), ((FAR, 0), (NEAR, 0)), ((FAR, 2), (NEAR, 2)))


def lagrange(coordinate):
    basis_values = []
    for row_node in range(4):
        weighted = jnp.ones_like(coordinate)
        for other_node in range(4):
            if other_node != row_node:
                weighted = weighted * (
                    (coordinate - NODE_COORD[other_node])
                    * (1.0 / (NODE_COORD[row_node] - NODE_COORD[other_node]))
                )
        basis_values.append(weighted)
    return basis_values


def bf16_parts(x):
    high = x.astype(jnp.bfloat16)
    low = (x - high.astype(jnp.float32)).astype(jnp.bfloat16)
    return high, low


def packed(x):
    rows, width = x.shape
    if width % LANES != LANES // 2:
        return x
    tiles = [x[:, i:i + LANES] for i in range(0, width - LANES // 2, LANES)]
    rest = x[:, width - LANES // 2:]
    return jnp.concatenate(tiles + [jnp.concatenate([rest[:rows // 2], rest[rows // 2:]], 1)], 0)


def packed_shape(rows, width):
    return (rows * width // LANES, LANES) if width % LANES == LANES // 2 else (rows, width)


def unpacked(dense, rows, width):
    if width % LANES != LANES // 2:
        return [(slice(0, rows), slice(0, width), dense)]
    parts = []
    for i in range(width // LANES):
        parts.append((slice(0, rows), slice(i * LANES, (i + 1) * LANES), dense[i * rows:(i + 1) * rows]))
    rest = dense[width // LANES * rows:]
    lanes = slice(width - LANES // 2, width)
    parts.append((slice(0, rows // 2), lanes, rest[:, :LANES // 2]))
    parts.append((slice(rows // 2, rows), lanes, rest[:, LANES // 2:]))
    return parts


def prep_kernel(counts_in, order_in, elem_in, coords_in, field_in, *rest):
    groups, capacity = elem_in.shape[1:]
    elements = field_in.shape[1]
    chips = groups // 2
    messages, rest = rest[:3], rest[3:]
    node_out, elem_out, dense, padded, starts, counts, order, elem, coords, field, sems = rest
    arrivals = [
        pltpu.make_async_copy(source, target, sems.at[i])
        for i, (source, target) in enumerate(
            (
                (counts_in, counts), (order_in, order), (elem_in, elem), (coords_in, coords),
                (field_in, field),
            )
        )
    ]
    for arrival in arrivals:
        arrival.start()
    for arrival in arrivals[:4]:
        arrival.wait()
    points = order.shape[1]
    padded[:, :points] = jnp.broadcast_to(order[...], (8, points))
    offset = jnp.int32(0)
    for k in range(3 * groups):
        starts[k] = offset
        offset = offset + counts[0, k]
    odd = lax.bitwise_and(lax.axis_index("sfc"), 1)
    me = lax.axis_index("grp")
    chip, core = lax.shift_right_logical(me, 1), lax.bitwise_and(me, 1)
    sides = (2 * odd, 2 - 2 * odd, 1)
    lane = lax.broadcasted_iota(jnp.int32, (8, capacity), 1)
    width = capacity + LANES
    for stage, d in enumerate(sides):
        message = messages[stage]
        for slot in range(groups):
            h = lax.rem(chip + slot // 2, chips) * 2 + lax.bitwise_xor(core, slot % 2)
            k = d * groups + h
            first, count = starts[k], counts[0, k]
            base = pl.multiple_of(lax.shift_left(lax.shift_right_logical(first, 7), 7), LANES)
            skip = lax.bitwise_and(first, LANES - 1)
            window = padded[:, pl.ds(base, width)]
            point = pltpu.roll(window, lax.rem(width - skip, width), 1)[:, :capacity]
            used = lane < count
            node = ((point.astype(jnp.float32) + 0.5) * (1.0 / elements)).astype(jnp.int32)
            at_elem = point - node * elements
            row, column = lax.shift_right_logical(node, 2), lax.bitwise_and(node, 3)
            inner_row = (row == 1) | (row == 2)
            inner_column = (column == 1) | (column == 2)
            weight = jnp.where(inner_row, NODE_WEIGHT[1], NODE_WEIGHT[0]) * jnp.where(
                inner_column, NODE_WEIGHT[1], NODE_WEIGHT[0]
            )
            weight = jnp.where(used, weight, 0.0)
            message[slot, 0:1, :] = elem[d, pl.ds(h, 1), :].astype(jnp.float32)
            message[slot, 1:2, :] = coords[0, d, pl.ds(h, 1), :]
            message[slot, 2:3, :] = coords[1, d, pl.ds(h, 1), :]
            message[slot, 3:4, :] = weight[0:1, :]
            node_out[stage, slot:slot + 1, :] = jnp.where(used, node, -1)[0:1, :]
            elem_out[stage, slot:slot + 1, :] = jnp.where(used, at_elem, -1)[0:1, :]
    arrivals[4].wait()
    dense[...] = packed(field[...])


def split_parts(dense, high, low):
    for rows, lanes, part in unpacked(dense[...], *high.shape):
        high[rows, lanes], low[rows, lanes] = bf16_parts(part)


def split_kernel(channels, mine, other, high_out, low_out, mass_out):
    for half, dense in enumerate((mine, other)):
        split_parts(dense, high_out.at[half], low_out.at[half])
    mass = None
    for part_rows, _, part in unpacked(mine[...], *high_out.shape[1:]):
        total = None
        for node in range(part_rows.start // channels, part_rows.stop // channels):
            at = node * channels - part_rows.start
            term = part[at:at + channels, :] * (NODE_WEIGHT[node // 4] * NODE_WEIGHT[node % 4])
            total = term if total is None else total + term
        summed = jnp.sum(total, axis=1, keepdims=True)
        mass = summed if mass is None else mass + summed
    mass_out[...] = mass + jnp.zeros((channels, LANES), jnp.float32)


def answered(channels, query, high, low):
    elements, capacity = high.shape[1], query.shape[-1]
    row = lax.broadcasted_iota(jnp.int32, (elements, capacity), 0).astype(jnp.float32)
    onehot = jnp.where(row == query[0:1, :], 1.0, 0.0).astype(jnp.bfloat16)
    field = jnp.dot(high[...], onehot, preferred_element_type=jnp.float32) + jnp.dot(
        low[...], onehot, preferred_element_type=jnp.float32
    )
    along_first = lagrange(query[1:2, :])
    along_second = lagrange(query[2:3, :])
    total = least = greatest = None
    for node in range(16):
        plane = field[node * channels:(node + 1) * channels, :]
        weighted = (along_first[node // 4] * along_second[node % 4]) * plane
        if total is None:
            total, least, greatest = weighted, plane, plane
        else:
            total = total + weighted
            least = jnp.minimum(least, plane)
            greatest = jnp.maximum(greatest, plane)
    value = jnp.minimum(jnp.maximum(total, least), greatest)
    return value, lane_sums(value * query[3:4, :])


def early_kernel(channels, high, low, carried, queries, values, mass):
    new = carried[...]
    for slot in range(2):
        values[slot], part = answered(channels, queries[slot], high.at[slot], low.at[slot])
        new = new + part
    mass[...] = new


def cross_kernel(*rest):
    *denses, high, low = rest
    for i, dense in enumerate(denses):
        split_parts(dense, high.at[i], low.at[i])


def late_kernel(channels, last, high, low, carried, queries, *rest):
    if last:
        old, values, mass = rest
    else:
        values, mass = rest
    new = carried[...]
    for i in range(values.shape[0]):
        values[i], part = answered(channels, queries[i + 2], high.at[i], low.at[i])
        new = new + part
    if not last:
        mass[...] = new
        return
    new = jnp.sum(new, axis=1, keepdims=True) + jnp.zeros((channels, LANES), jnp.float32)
    lane = lax.broadcasted_iota(jnp.int32, (channels, LANES), 1)
    which = lax.broadcasted_iota(jnp.int32, (channels, LANES), 0)
    spread = jnp.where(lane == which, old[...], 0.0) + jnp.where(lane == which + channels, new, 0.0)
    mass[...] = jnp.broadcast_to(jnp.sum(spread, axis=0, keepdims=True), mass.shape)


def scatter_kernel(channels, plan, *rest):
    values, (node, elem), rest = rest[:len(plan)], rest[len(plan):len(plan) + 2], rest[len(plan) + 2:]
    *carried, out = rest
    elements, capacity = out.shape[1], elem.shape[-1]
    row = lax.broadcasted_iota(jnp.int32, (elements, capacity), 0)
    total = None
    for (stage, first), block in zip(plan, values):
        for i in range(block.shape[0]):
            slot = slice(first + i, first + i + 1)
            at_node = jnp.broadcast_to(
                node[stage, slot, :].astype(jnp.float32), (channels, capacity)
            ).astype(jnp.bfloat16)
            onehot = jnp.where(row == elem[stage, slot, :], 1.0, 0.0).astype(jnp.bfloat16)
            for part in bf16_parts(block[i]):
                zero = jnp.zeros_like(part)
                spread = jnp.concatenate(
                    [jnp.where(at_node == float(n), part, zero) for n in range(16)], 0
                )
                term = lax.dot_general(
                    spread, onehot, (((1,), (1,)), ((), ())), preferred_element_type=jnp.float32
                )
                total = term if total is None else total + term
    out[...] = total + carried[0][...] if carried else total


def lane_sums(x):
    return sum(x[:, i:i + LANES] for i in range(0, x.shape[1], LANES))


def scale_kernel(channels, carried, masses, out):
    total = jnp.sum(masses[...], axis=0, keepdims=True)
    lane = lax.broadcasted_iota(jnp.int32, (channels, LANES), 1)
    which = lax.broadcasted_iota(jnp.int32, (channels, LANES), 0)
    old = jnp.sum(jnp.where(lane == which, total, 0.0), axis=1, keepdims=True)
    new = jnp.sum(jnp.where(lane == which + channels, total, 0.0), axis=1, keepdims=True)
    ratio = old / new
    for n in range(16):
        rows = slice(n * channels, (n + 1) * channels)
        out[rows, :] = carried[rows, :] * ratio


def whole(memory=VMEM):
    return pl.BlockSpec(memory_space=memory)


def call(kernel, out_shape, *args, outside=0, scratch=(), flops=1_000_000):
    outs = out_shape if isinstance(out_shape, (list, tuple)) else [out_shape]
    moved = sum(x.size * x.dtype.itemsize for x in list(args) + list(outs))
    run = pl.pallas_call(
        kernel,
        out_shape=out_shape,
        in_specs=[whole(HBM)] * outside + [whole()] * (len(args) - outside),
        out_specs=[whole()] * len(outs) if outs is out_shape else whole(),
        scratch_shapes=list(scratch),
        compiler_params=pltpu.CompilerParams(vmem_limit_bytes=16 * 1024 * 1024),
        cost_estimate=pl.CostEstimate(flops=flops, bytes_accessed=moved, transcendentals=0),
    )
    return run(
        *[pltpu.with_memory_space_constraint(x, HBM) if i < outside else x for i, x in enumerate(args)]
    )


def local(tracers, send_counts, point_order, depart_elem, depart_coords):
    node_count, levels, tracer_count, elements = tracers.shape
    channels = levels * tracer_count
    segments, groups = lax.axis_size("sfc"), lax.axis_size("grp")
    chips = groups // 2
    devices = segments * groups
    capacity = depart_elem.shape[-1]
    rows, points = node_count * channels, node_count * elements
    f32, i32, bf16 = jnp.float32, jnp.int32, jnp.bfloat16
    shape = jax.ShapeDtypeStruct
    dense_shape = packed_shape(rows, elements)

    def sent(stage, x):
        if stage == OWN:
            return x
        pairs = [(s, (((s + 1) ^ 1) - 1) % segments if stage == FAR else s ^ 1) for s in range(segments)]
        return lax.ppermute(x, "sfc", pairs)

    *queries, node, elem, dense = call(
        prep_kernel,
        [shape((groups, 4, capacity), f32)] * 3
        + [shape((3, groups, capacity), i32)] * 2
        + [shape(dense_shape, f32)],
        send_counts.reshape(1, 3 * groups),
        point_order.reshape(1, points),
        depart_elem.reshape(3, groups, capacity),
        depart_coords.reshape(2, 3, groups, capacity),
        tracers.reshape(rows, elements),
        outside=5,
        scratch=[
            pltpu.VMEM((8, points + capacity + LANES), i32),
            pltpu.SMEM((3 * groups,), i32),
            pltpu.SMEM((1, 3 * groups), i32),
            pltpu.VMEM((1, points), i32),
            pltpu.VMEM((3, groups, capacity), i32),
            pltpu.VMEM((2, 3, groups, capacity), f32),
            pltpu.VMEM((rows, elements), f32),
            pltpu.SemaphoreType.DMA((5,)),
        ],
    )
    other_core = [(i, i ^ 1) for i in range(groups)]
    reached = []
    for hop in range(1, chips):
        reached.append(
            lax.ppermute(dense, "grp", [((i + 2 * hop) % groups, i) for i in range(groups)])
        )
    queries = [sent(stage, queries[stage]) for stage in range(3)]
    partner = lax.ppermute(dense, "grp", other_core)
    high, low, old = call(
        functools.partial(split_kernel, channels),
        [shape((2, rows, elements), bf16)] * 2 + [shape((channels, LANES), f32)],
        dense,
        partner,
    )
    new = jnp.zeros((channels, LANES), f32)
    sums = shape((channels, LANES), f32)
    early, late = [], []
    for stage in range(3):
        values, new = call(
            functools.partial(early_kernel, channels),
            [shape((2, channels, capacity), f32), sums],
            high, low, new, queries[stage],
            flops=200_000_000,
        )
        early.append(sent(stage, values))
    across = []
    for hop, x in enumerate(reached, 1):
        across += [x, lax.ppermute(x, "grp", other_core)]
    far_high, far_low = call(cross_kernel, [shape((groups - 2, rows, elements), bf16)] * 2, *across)
    for stage in range(3):
        last = stage == 2
        values, new = call(
            functools.partial(late_kernel, channels, last),
            [
                shape((groups - 2, channels, capacity), f32),
                shape((devices, LANES), f32) if last else sums,
            ],
            far_high, far_low, new, queries[stage], *([old] if last else []),
            flops=200_000_000,
        )
        late.append(sent(stage, values))
    masses = lax.all_to_all(
        new.reshape(devices, 1, LANES), ("sfc", "grp"), split_axis=0, concat_axis=0, tiled=True
    )
    so_far = []
    for plan in SCATTERS:
        blocks = [(early if first == 0 else late)[stage] for stage, first in plan]
        so_far = [
            call(
                functools.partial(scatter_kernel, channels, plan),
                shape((rows, elements), f32),
                *blocks, node, elem, *so_far,
                flops=400_000_000,
            )
        ]
    out = call(
        functools.partial(scale_kernel, channels),
        shape((rows, elements), f32),
        *so_far, masses.reshape(devices, LANES),
    )
    return out.reshape(tracers.shape)


def solution(mesh):
    in_specs = (
        P(None, None, None, ("sfc", "grp")),
        P("sfc", "grp", None),
        P("sfc", "grp", None),
        P("sfc", "grp", None, None, None),
        P("sfc", "grp", None, None, None, None),
    )
    out_specs = P(None, None, None, ("sfc", "grp"))

    return jax.shard_map(local, mesh=mesh, in_specs=in_specs, out_specs=out_specs, check_vma=False)
```
